32 devices in a mesh: dp: 8 (over y, x, core), tp: 4 (over z).
Axes of the slice: x: 2, y: 2, z: 4, core: 2. Of those that a mesh axis runs over, the one named last changes fastest.
Arguments:
- resid: bfloat16 [2048, 4096], P('dp'), may hold values from -6 to 6
- gain: bfloat16 [4096], replicated, may hold values from 0.25 to 1.75
- grad_q: bfloat16 [2048, 3072], P('dp', 'tp'), may hold values from -1.25 to 1.25
- w_query: bfloat16 [3072, 4096], P('tp'), may hold values from -0.375 to 0.375
- grad_in: bfloat16 [2048, 4096], P('dp'), may hold values from -2 to 2
Outputs:
- weight_grad: float32 [3072, 4096], P(('tp', 'dp'))
- gain_grad: float32 [4096], replicated
- grad_out: bfloat16 [2048, 4096], P('dp')
The draws below stay inside these ranges and needn't reach their ends.
All inputs are finite; a program needn't handle non-finite values.
Results may differ from the reference program's by a relative error of at most 0.014.
Values may be sent and summed in bfloat16 or wider, within the bound.
A program may use at most 128 MiB of HBM per device.

```python
import jax
import jax.numpy as jnp
from jax import lax

D = 4096
QW = 3072
TOKENS = 2048
N_TP = 4


def with_spikes(drawn, stream_key, source, target, parts, factor):
    owner, partner = [(jnp.arange(drawn.shape[dim]) // (drawn.shape[dim] // parts)).reshape([-1 if axis == dim else 1 for axis in range(drawn.ndim)]) for dim in (source, target)]
    chosen = jax.random.permutation(stream_key, parts)[partner]
    strong = (owner == chosen) | (owner == (partner + parts // 2) % parts)
    return jnp.where(strong, factor * drawn, drawn)


def shard_levels(key, dims, cuts, low, top_value):
    def one(dim, parts):
        draws = jax.random.uniform(jax.random.fold_in(jax.random.fold_in(key, 6), dim), (parts,), jnp.float32, low / len(cuts), top_value / len(cuts))
        return jnp.repeat(jnp.exp(draws), dims[dim] // parts).reshape((-1,) + (1,) * (len(dims) - dim - 1))

    level = one(*cuts[0])
    for cut in cuts[1:]:
        level = level * one(*cut)
    return level


def gaussian(own_key, extent, scale, bound, split=(), dtype=jnp.bfloat16):
    drawn = scale * jax.random.normal(own_key, extent, jnp.float32)
    if split:
        drawn = drawn * shard_levels(own_key, extent, split, -0.22, 0.18)
    return jnp.clip(drawn, -bound, bound).astype(dtype)


def gaussian_with(stream_key, dims, deviation, reach, split, heavy, kind=jnp.bfloat16):
    values = deviation * jax.random.normal(stream_key, dims, jnp.float32)
    if split:
        values = values * shard_levels(stream_key, dims, split, -0.22, 0.18)
    return jnp.clip(with_spikes(values, jax.random.fold_in(stream_key, 3), *heavy), -reach, reach).astype(kind)


def setup_inputs(seed: int = 0) -> dict:
    streams_of = jax.random.split(jax.random.key(seed), 6)
    resid = gaussian(streams_of[0], (TOKENS, D), 1.0, 6.0, ((0, 8),))
    gain = jnp.clip(1.0 + 0.15 * jax.random.normal(streams_of[1], (D,), jnp.float32), 0.25, 1.75).astype(jnp.bfloat16)
    grad_q = gaussian_with(streams_of[2], (TOKENS, QW), 0.0625, 1.25, ((0, 8), (1, 4)), (0, 1, 8, 2.0))
    w_query = gaussian(streams_of[3], (QW, D), (D // 16) ** -0.5, 0.375, ((0, 4),))
    grad_in = gaussian(streams_of[4], (TOKENS, D), 0.125, 2.0, ((0, 8),))
    return dict(resid=resid, gain=gain, grad_q=grad_q, w_query=w_query, grad_in=grad_in)


def reference(resid, gain, grad_q, w_query, grad_in):
    resid_f = resid.astype(jnp.float32)
    gain_f = gain.astype(jnp.float32)
    inv_rms = lax.rsqrt(lax.optimization_barrier(jnp.mean(resid_f * resid_f, axis=-1, keepdims=True)) + 1e-05)
    unit = resid_f * inv_rms
    normed = (unit * gain_f).astype(jnp.bfloat16)
    weight_grad = jnp.dot(grad_q.astype(jnp.float32).T, normed.astype(jnp.float32), preferred_element_type=jnp.float32)
    block = QW // N_TP
    dnormed = jnp.zeros(resid.shape, jnp.float32)
    for index in range(N_TP):
        cols = grad_q[:, index * block:(index + 1) * block].astype(jnp.float32)
        rows = w_query[index * block:(index + 1) * block, :].astype(jnp.float32)
        partial_value = jnp.dot(cols, rows, preferred_element_type=jnp.float32).astype(jnp.bfloat16)
        dnormed = dnormed + partial_value.astype(jnp.float32)
    gain_grad = lax.optimization_barrier(jnp.sum(dnormed * unit, axis=0))
    dunit = dnormed * gain_f
    inner = lax.optimization_barrier(jnp.mean(dunit * unit, axis=-1, keepdims=True))
    grad_out = (grad_in.astype(jnp.float32) + inv_rms * (dunit - unit * inner)).astype(jnp.bfloat16)
    return (weight_grad, gain_grad, grad_out)
```

```python
import functools

import jax
import jax.numpy as jnp
from jax import lax
from jax.experimental import pallas as pl
from jax.experimental.pallas import tpu as pltpu
from jax.sharding import PartitionSpec as P

MESH = pl.DeviceIdType.MESH
F32 = jnp.float32
BF16 = jnp.bfloat16
ROWS = 16
TILES = 8
QUARTERS = 4
FIRST = 2
LAG = 4


def norm_rows(rows_bf, gain_f):
    rows_f = rows_bf.astype(jnp.float32)
    inv_rms = lax.rsqrt(jnp.mean(rows_f * rows_f, axis=-1, keepdims=True) + 1e-05)
    unit = rows_f * inv_rms
    return (inv_rms, unit, (unit * gain_f).astype(jnp.bfloat16))


def per_device(resid, gain, grad_q, w_query, grad_in):
    gain_f = gain.astype(jnp.float32)
    inv_rms, unit, normed = norm_rows(resid, gain_f)
    local_term = jnp.dot(grad_q, w_query, preferred_element_type=jnp.float32)
    dnormed = lax.psum(local_term.astype(jnp.bfloat16), "tp").astype(jnp.float32)
    full_grad = lax.dot_general(
        grad_q, normed, (((0,), (0,)), ((), ())), preferred_element_type=jnp.float32
    )
    weight_grad = lax.psum_scatter(full_grad, "dp", scatter_dimension=0, tiled=True)
    gain_grad = lax.psum(jnp.sum(dnormed * unit, axis=0), "dp")
    dunit = dnormed * gain_f
    inner = jnp.mean(dunit * unit, axis=-1, keepdims=True)
    grad_rows = (grad_in.astype(jnp.float32) + inv_rms * (dunit - unit * inner)).astype(
        jnp.bfloat16
    )
    return (weight_grad, gain_grad, grad_rows)


def kernel(n_dp, n_tp, resid, gain, grad_q, w_query, grad_in, wg_out, gg_out, go_out,
           wv, rv, gqv, giv, nv, part, from_mate, from_peer, ds, gov, gain_f, inv, gq_t, gq_p,
           fgs, fgr, keep, xs, xr, ys, yr, wgo, gacc, gslot, gz,
           w_sem, in_sem, r_sem, gi_sem, so, sp, rm, rp, out_sem,
           s1, r1, s2, r2, s3, r3, wg_sem, sg, rg, sz, rz):
    dp, tp = lax.axis_index("dp"), lax.axis_index("tp")
    _, tokens, span = rv.shape
    heads = gqv.shape[1]
    width = QUARTERS * span
    chunks = tokens // ROWS
    cols = width // TILES
    block = heads // n_dp
    h = tp // 2
    is_inner = jnp.logical_and(tp > 0, tp < n_tp - 1)
    is_outer = jnp.logical_not(is_inner)
    mate = jnp.where(is_inner, h * (n_tp - 1), 1 + h)
    peer = 2 - h
    core, xx, yy = dp % 2, (dp // 2) % 2, dp // 4
    core_mate = dp + 1 - 2 * core
    x_mate = dp + 2 - 4 * xx
    y_mate = dp + 4 - 8 * yy
    own, other = 2 * h, 2 - 2 * h
    turns = ((other, 0), (own, 0), (other, 1), (own, 1))

    def span_of(a):
        return pl.ds(pl.multiple_of(a * span, span), span)

    def w_copy(s):
        a = turns[s][0] + turns[s][1]
        return pltpu.make_async_copy(w_query.at[:, span_of(a)], wv.at[a], w_sem.at[s])

    def r_copy(a):
        return pltpu.make_async_copy(
            resid.at[:, a * span:(a + 1) * span], rv.at[a], r_sem.at[a])

    def gi_copy(a):
        return pltpu.make_async_copy(
            grad_in.at[:, a * span:(a + 1) * span], giv.at[a], gi_sem.at[a])

    gq_copy = pltpu.make_async_copy(grad_q, gqv, in_sem.at[0])
    gq_copy.start()
    for s in range(QUARTERS):
        w_copy(s).start()

    barrier = pltpu.get_barrier_semaphore()
    for to in (core_mate, x_mate, y_mate):
        pl.semaphore_signal(barrier, inc=1, device_id={"dp": to}, device_id_type=MESH)
    pl.semaphore_signal(barrier, inc=1, device_id={"tp": mate}, device_id_type=MESH)

    @pl.when(is_inner)
    def _():
        pl.semaphore_signal(barrier, inc=1, device_id={"tp": peer}, device_id_type=MESH)

    def rows_of(c):
        return pl.ds(pl.multiple_of(c * ROWS, ROWS), ROWS)

    def to_mate(src, dst, a, c):
        return pltpu.make_async_remote_copy(
            src_ref=src.at[a, rows_of(c)], dst_ref=dst.at[a, rows_of(c)],
            send_sem=so.at[0], recv_sem=rm.at[QUARTERS * c + a],
            device_id={"tp": mate}, device_id_type=MESH)

    def to_peer(src, dst, a, c):
        return pltpu.make_async_remote_copy(
            src_ref=src.at[a, rows_of(c)], dst_ref=dst.at[a, rows_of(c)],
            send_sem=sp.at[0], recv_sem=rp.at[QUARTERS * c + a],
            device_id={"tp": peer}, device_id_type=MESH)

    def hop(src, dst, send, recv, t, to):
        return pltpu.make_async_remote_copy(
            src_ref=src.at[t], dst_ref=dst.at[t], send_sem=send.at[t], recv_sem=recv.at[t],
            device_id={"dp": to}, device_id_type=MESH)

    gq_copy.wait()
    head = FIRST * ROWS
    for s, (base, q) in enumerate(turns):
        a = base + q
        w_copy(s).wait()
        part[a, :head, :] = jnp.dot(
            gqv[:head, :], wv[a], preferred_element_type=F32).astype(BF16)
        if s == 0:
            @pl.when(is_inner)
            def _():
                pl.semaphore_wait(barrier, 5)

            @pl.when(is_outer)
            def _():
                pl.semaphore_wait(barrier, 4)

        @pl.when(is_outer)
        def _():
            for c in range(FIRST):
                to_mate(part, from_mate, a, c).start()

    for a in range(QUARTERS):
        r_copy(a).start()
    for a in range(QUARTERS):
        gi_copy(a).start()

    for base, q in turns:
        a = base + q
        part[a, head:, :] = jnp.dot(
            gqv[head:, :], wv[a], preferred_element_type=F32).astype(BF16)

    @pl.when(is_outer)
    def _():
        @pl.loop(FIRST, chunks)
        def _(c):
            for base in (other, own):
                for q in range(2):
                    to_mate(part, from_mate, base + q, c).start()

    for a in range(QUARTERS):
        gain_f[a] = gain[:, a * span:(a + 1) * span].astype(F32)
        r_copy(a).wait()
        gi_copy(a).wait()
    gacc[...] = jnp.zeros_like(gacc)

    def norm(c):
        r = rows_of(c)
        total = jnp.zeros((ROWS, span), F32)
        for a in range(QUARTERS):
            x = rv[a, r, :].astype(F32)
            total = total + x * x
        scale = lax.rsqrt(jnp.sum(total, axis=-1, keepdims=True) * (1.0 / width) + 1e-05)
        inv[r, :] = scale
        for a in range(QUARTERS):
            nv[a, r, :] = (rv[a, r, :].astype(F32) * scale * gain_f[a]).astype(BF16)

    def regroup():
        gq_t[...] = gqv[...].T
        for v in range(2):
            for j, rel in enumerate(((0, 2, 1, 3), (0, 1, 2, 3))[v]):
                y_to = yy + (rel // 2) * (1 - 2 * yy)
                x_to = xx + (rel % 2) * (1 - 2 * xx)
                for mine in range(2):
                    c_to = core if mine else 1 - core
                    at = pl.multiple_of((y_to * 4 + x_to * 2 + c_to) * block, block)
                    gq_p[v, mine, j * block:(j + 1) * block, :] = gq_t[pl.ds(at, block), :]

    first, second = (x_mate, y_mate), (y_mate, x_mate)

    def product(mine, j, v):
        return jnp.dot(gq_p[v, mine], nv[j, :, v * cols:(v + 1) * cols], preferred_element_type=F32)

    def stage1(j):
        for v in range(2):
            t = 2 * j + v
            fgs[t] = product(0, j, v).astype(BF16)
            hop(fgs, fgr, s1, r1, t, core_mate).start()

    def stage2(j):
        for v in range(2):
            t = 2 * j + v
            hop(fgs, fgr, s1, r1, t, core_mate).wait_recv()
            total = product(1, j, v) + fgr[t].astype(F32)
            xs[t] = total[2 * block:].astype(BF16)
            hop(xs, xr, s2, r2, t, first[v]).start()
            keep[t] = total[:2 * block]

    def stage3(j):
        for v in range(2):
            t = 2 * j + v
            hop(xs, xr, s2, r2, t, first[v]).wait_recv()
            ys[t] = (keep[t, block:] + xr[t, block:].astype(F32)).astype(BF16)
            hop(ys, yr, s3, r3, t, second[v]).start()
            keep[t, :block] = keep[t, :block] + xr[t, :block].astype(F32)

    def wg_copy(t):
        return pltpu.make_async_copy(
            wgo.at[t], wg_out.at[:, pl.ds(pl.multiple_of(t * cols, cols), cols)], wg_sem.at[t])

    def stage4(j):
        for v in range(2):
            t = 2 * j + v
            hop(ys, yr, s3, r3, t, second[v]).wait_recv()
            wgo[t] = keep[t, :block] + yr[t].astype(F32)
            wg_copy(t).start()

    def pass_on(c):
        for q in range(2):
            a = other + q
            to_mate(part, from_mate, a, c).wait_recv()
            r = rows_of(c)
            part[a, r, :] = (
                part[a, r, :].astype(F32) + from_mate[a, r, :].astype(F32)).astype(BF16)
            to_peer(part, from_peer, a, c).start()

    def root(c):
        for q in range(2):
            a = own + q
            to_mate(part, from_mate, a, c).wait_recv()
            to_peer(part, from_peer, a, c).wait_recv()
            r = rows_of(c)
            dnormed = part[a, r, :].astype(F32) + from_mate[a, r, :].astype(F32)
            dnormed = dnormed + from_peer[a, r, :].astype(F32)
            ds[a, r, :] = dnormed.astype(BF16)
            to_mate(ds, ds, a, c).start()
            to_peer(ds, ds, a, c).start()
            term = dnormed * (rv[a, r, :].astype(F32) * inv[r, :])
            gacc[q] += term[:8] + term[8:]

    def forward(c):
        for q in range(2):
            a = other + q
            to_peer(ds, ds, a, c).wait_recv()
            to_mate(ds, ds, a, c).start()

    def collect(c):
        for a in range(QUARTERS):
            to_mate(part, ds, a, c).wait_recv()

    def out_copy(a, c):
        return pltpu.make_async_copy(
            gov.at[a, rows_of(c)], go_out.at[rows_of(c), a * span:(a + 1) * span],
            out_sem.at[QUARTERS * c + a])

    def finish(c):
        r = rows_of(c)
        scale = inv[r, :]
        total = jnp.zeros((ROWS, span), F32)
        for a in range(QUARTERS):
            total = total + ds[a, r, :].astype(F32) * gain_f[a] * (rv[a, r, :].astype(F32) * scale)
        mean = jnp.sum(total, axis=-1, keepdims=True) * (1.0 / width)
        for a in range(QUARTERS):
            dunit = ds[a, r, :].astype(F32) * gain_f[a]
            unit = rv[a, r, :].astype(F32) * scale
            gov[a, r, :] = (
                giv[a, r, :].astype(F32) + scale * (dunit - unit * mean)).astype(BF16)
            out_copy(a, c).start()

    def g_copy(o):
        return pltpu.make_async_remote_copy(
            src_ref=gslot.at[0], dst_ref=gslot.at[o], send_sem=sg.at[o], recv_sem=rg.at[o],
            device_id={"dp": (dp + o) % n_dp}, device_id_type=MESH)

    targets = (mate, peer, (1 - h) * (n_tp - 1))

    def z_copy(i):
        return pltpu.make_async_remote_copy(
            src_ref=gz.at[h], dst_ref=gz.at[h], send_sem=sz.at[i], recv_sem=rz.at[h],
            device_id={"tp": targets[i]}, device_id_type=MESH)

    def z_wait(which):
        pltpu.make_async_remote_copy(
            src_ref=gz.at[which], dst_ref=gz.at[which], send_sem=sz.at[0], recv_sem=rz.at[which],
            device_id={"tp": mate}, device_id_type=MESH).wait_recv()

    def at(i, lo, hi):
        return jnp.logical_and(i >= lo, i < hi)

    @pl.loop(0, chunks + LAG)
    def _(i):
        @pl.when(jnp.logical_and(is_inner, i < chunks))
        def _():
            pass_on(i)

        @pl.when(jnp.logical_and(is_inner, at(i, 1, chunks + 1)))
        def _():
            root(i - 1)

        @pl.when(jnp.logical_and(is_inner, i == chunks))
        def _():
            for q in range(2):
                gslot[0, q:q + 1, :] = jnp.sum(gacc[q], axis=0, keepdims=True)
            for o in range(1, n_dp):
                g_copy(o).start()

        @pl.when(jnp.logical_and(is_inner, at(i, 2, chunks + 2)))
        def _():
            forward(i - 2)

        @pl.when(jnp.logical_and(is_inner, at(i, 3, chunks + 3)))
        def _():
            finish(i - 3)

        @pl.when(jnp.logical_and(is_outer, i >= LAG))
        def _():
            collect(i - LAG)
            finish(i - LAG)

        @pl.when(i == 0)
        def _():
            pl.loop(0, 9)(norm)

        @pl.when(i == 1)
        def _():
            pl.loop(9, 13)(norm)

        @pl.when(i == 2)
        def _():
            pl.loop(13, chunks)(norm)
            regroup()

        @pl.when(at(i, 3, 5))
        def _():
            stage1(2 * (i - 3))
            stage1(2 * (i - 3) + 1)

        @pl.when(at(i, 5, 9))
        def _():
            stage2(i - 5)

        @pl.when(at(i, 9, 13))
        def _():
            stage3(i - 9)

        @pl.when(at(i, 13, 17))
        def _():
            stage4(i - 13)

    @pl.when(is_inner)
    def _():
        for o in range(1, n_dp):
            g_copy(o).wait_recv()
        total = gslot[dp % n_dp]
        for d in range(1, n_dp):
            total = total + gslot[(dp + n_dp - d) % n_dp]
        gz[h] = total
        for i in range(3):
            z_copy(i).start()
        z_wait(1 - h)
        for i in range(3):
            z_copy(i).wait_send()
        for o in range(1, n_dp):
            g_copy(o).wait_send()
        pltpu.make_async_remote_copy(
            src_ref=part, dst_ref=ds, send_sem=sp.at[0], recv_sem=rp.at[0],
            device_id={"tp": peer}, device_id_type=MESH).wait_send()

    @pl.when(is_outer)
    def _():
        z_wait(0)
        z_wait(1)

    for a in range(QUARTERS):
        gg_out[:, a * span:(a + 1) * span] = gz[a // 2, a % 2:a % 2 + 1, :]
    pltpu.make_async_remote_copy(
        src_ref=part, dst_ref=ds, send_sem=so.at[0], recv_sem=rm.at[0],
        device_id={"tp": mate}, device_id_type=MESH).wait_send()

    @pl.loop(0, chunks)
    def _(c):
        for a in range(QUARTERS):
            out_copy(a, c).wait()

    for t in range(TILES):
        hop(fgs, fgr, s1, r1, t, core_mate).wait_send()
        hop(xs, xr, s2, r2, t, first[t % 2]).wait_send()
        hop(ys, yr, s3, r3, t, second[t % 2]).wait_send()
        wg_copy(t).wait()


def fused(n_dp, n_tp, resid, gain, grad_q, w_query, grad_in):
    tokens, width = resid.shape
    heads = grad_q.shape[1]
    chunks = tokens // ROWS
    block, cols, span = heads // n_dp, width // TILES, width // QUARTERS
    any_space = pl.BlockSpec(memory_space=pl.ANY)
    vmem = pl.BlockSpec(memory_space=pltpu.VMEM)
    dma = lambda n: pltpu.SemaphoreType.DMA((n,))
    wide = lambda: pltpu.VMEM((QUARTERS, tokens, span), BF16)
    weight_grad, gain_grad, grad_rows = pl.pallas_call(
        functools.partial(kernel, n_dp, n_tp),
        out_shape=(
            jax.ShapeDtypeStruct((block, width), F32),
            jax.ShapeDtypeStruct((1, width), F32),
            jax.ShapeDtypeStruct((tokens, width), BF16),
        ),
        in_specs=[any_space, vmem, any_space, any_space, any_space],
        out_specs=(any_space, vmem, any_space),
        scratch_shapes=[
            pltpu.VMEM((QUARTERS, heads, span), BF16),
            wide(),
            pltpu.VMEM((tokens, heads), BF16),
            wide(), wide(), wide(), wide(), wide(), wide(), wide(),
            pltpu.VMEM((QUARTERS, 1, span), F32),
            pltpu.VMEM((tokens, 1), F32),
            pltpu.VMEM((heads, tokens), BF16),
            pltpu.VMEM((2, 2, 4 * block, tokens), BF16),
            pltpu.VMEM((TILES, 4 * block, cols), BF16),
            pltpu.VMEM((TILES, 4 * block, cols), BF16),
            pltpu.VMEM((TILES, 2 * block, cols), F32),
            pltpu.VMEM((TILES, 2 * block, cols), BF16),
            pltpu.VMEM((TILES, 2 * block, cols), BF16),
            pltpu.VMEM((TILES, block, cols), BF16),
            pltpu.VMEM((TILES, block, cols), BF16),
            pltpu.VMEM((TILES, block, cols), F32),
            pltpu.VMEM((2, 8, span), F32),
            pltpu.VMEM((n_dp, 2, span), F32),
            pltpu.VMEM((2, 2, span), F32),
            dma(QUARTERS), dma(1), dma(QUARTERS), dma(QUARTERS), dma(1), dma(1),
            dma(QUARTERS * chunks), dma(QUARTERS * chunks), dma(QUARTERS * chunks),
            dma(TILES), dma(TILES), dma(TILES), dma(TILES), dma(TILES), dma(TILES), dma(TILES),
            dma(n_dp), dma(n_dp), dma(3), dma(2),
        ],
        compiler_params=pltpu.CompilerParams(
            collective_id=0, has_side_effects=True, vmem_limit_bytes=60 * 1024 * 1024
        ),
    )(resid, gain.reshape(1, width), grad_q, w_query, grad_in)
    return weight_grad, gain_grad.reshape(width), grad_rows


def solution(mesh):
    n_dp, n_tp = mesh.shape["dp"], mesh.shape["tp"]
    if (n_dp, n_tp) == (2 * 2 * 2, 4):
        body = functools.partial(fused, n_dp, n_tp)
    else:
        body = per_device
    return jax.shard_map(
        body,
        mesh=mesh,
        in_specs=(P("dp", None), P(), P("dp", "tp"), P("tp", None), P("dp", None)),
        out_specs=(P(("tp", "dp"), None), P(), P("dp", None)),
        check_vma=False,
    )
```

```python
import functools

import jax
import jax.numpy as jnp
from jax import lax
from jax.experimental import pallas as pl
from jax.experimental.pallas import tpu as pltpu
from jax.sharding import PartitionSpec as P

MESH = pl.DeviceIdType.MESH
F32 = jnp.float32
BF16 = jnp.bfloat16
ROWS = 16
TILES = 8
QUARTERS = 4
LEAD = 2
FIRST = LEAD + 1
VMEM_MIB = 52
LAG = 6


def norm_rows(rows_bf, gain_f):
    rows_f = rows_bf.astype(jnp.float32)
    inv_rms = lax.rsqrt(jnp.mean(rows_f * rows_f, axis=-1, keepdims=True) + 1e-05)
    unit = rows_f * inv_rms
    return (inv_rms, unit, (unit * gain_f).astype(jnp.bfloat16))


def per_device(resid, gain, grad_q, w_query, grad_in):
    gain_f = gain.astype(jnp.float32)
    inv_rms, unit, normed = norm_rows(resid, gain_f)
    local_term = jnp.dot(grad_q, w_query, preferred_element_type=jnp.float32)
    dnormed = lax.psum(local_term.astype(jnp.bfloat16), "tp").astype(jnp.float32)
    full_grad = lax.dot_general(
        grad_q, normed, (((0,), (0,)), ((), ())), preferred_element_type=jnp.float32
    )
    weight_grad = lax.psum_scatter(full_grad, "dp", scatter_dimension=0, tiled=True)
    gain_grad = lax.psum(jnp.sum(dnormed * unit, axis=0), "dp")
    dunit = dnormed * gain_f
    inner = jnp.mean(dunit * unit, axis=-1, keepdims=True)
    grad_rows = (grad_in.astype(jnp.float32) + inv_rms * (dunit - unit * inner)).astype(
        jnp.bfloat16
    )
    return (weight_grad, gain_grad, grad_rows)


def kernel(n_dp, n_tp, resid, gain, grad_q, w_query, grad_in, wgo, ggv, gov,
           wv, rv, gqv, giv, nv, part, from_mate, from_peer, ds, gain_v, gain_f, inv, gq_t, gq_p,
           fgs, fgr, keep, xs, xr, ys, yr, gacc, gslot, gz,
           w_sem, in_sem, r_sem, gi_sem, so, sp, rm, rp,
           s1, r1, s2, r2, s3, r3, sg, rg, sz, rz):
    dp, tp = lax.axis_index("dp"), lax.axis_index("tp")
    _, tokens, span = rv.shape
    heads = gqv.shape[1]
    width = QUARTERS * span
    chunks = tokens // ROWS
    cols = width // TILES
    block = heads // n_dp
    h = tp // 2
    is_inner = jnp.logical_and(tp > 0, tp < n_tp - 1)
    is_outer = jnp.logical_not(is_inner)
    mate = jnp.where(is_inner, h * (n_tp - 1), 1 + h)
    peer = 2 - h
    core, xx, yy = dp % 2, (dp // 2) % 2, dp // 4
    core_mate = dp + 1 - 2 * core
    x_mate = dp + 2 - 4 * xx
    y_mate = dp + 4 - 8 * yy
    own, other = 2 * h, 2 - 2 * h
    turns = ((other, 0), (other, 1), (own, 0), (own, 1))

    def span_of(a):
        return pl.ds(pl.multiple_of(a * span, span), span)

    def w_copy(s):
        a = turns[s][0] + turns[s][1]
        return pltpu.make_async_copy(w_query.at[:, span_of(a)], wv.at[a], w_sem.at[s])

    def r_copy(a):
        return pltpu.make_async_copy(
            resid.at[:, a * span:(a + 1) * span], rv.at[a], r_sem.at[a])

    def gi_copy(a):
        return pltpu.make_async_copy(
            grad_in.at[:, a * span:(a + 1) * span], giv.at[a], gi_sem.at[a])

    gq_copy = pltpu.make_async_copy(grad_q, gqv, in_sem.at[0])
    gain_copy = pltpu.make_async_copy(gain, gain_v, in_sem.at[1])
    gq_copy.start()
    gain_copy.start()
    for s in range(QUARTERS):
        w_copy(s).start()

    barrier = pltpu.get_barrier_semaphore()
    for to in (core_mate, x_mate, y_mate):
        pl.semaphore_signal(barrier, inc=1, device_id={"dp": to}, device_id_type=MESH)
    pl.semaphore_signal(barrier, inc=1, device_id={"tp": mate}, device_id_type=MESH)

    @pl.when(is_inner)
    def _():
        pl.semaphore_signal(barrier, inc=1, device_id={"tp": peer}, device_id_type=MESH)

    def rows_of(c):
        return pl.ds(pl.multiple_of(c * ROWS, ROWS), ROWS)

    def to_mate(src, dst, base, c):
        return pltpu.make_async_remote_copy(
            src_ref=src.at[pl.ds(base, 2), rows_of(c)], dst_ref=dst.at[pl.ds(base, 2), rows_of(c)],
            send_sem=so.at[0], recv_sem=rm.at[2 * c + base // 2],
            device_id={"tp": mate}, device_id_type=MESH)

    def to_peer(src, dst, base, c):
        return pltpu.make_async_remote_copy(
            src_ref=src.at[pl.ds(base, 2), rows_of(c)], dst_ref=dst.at[pl.ds(base, 2), rows_of(c)],
            send_sem=sp.at[0], recv_sem=rp.at[2 * c + base // 2],
            device_id={"tp": peer}, device_id_type=MESH)

    def hop(src, dst, send, recv, t, to):
        return pltpu.make_async_remote_copy(
            src_ref=src.at[t], dst_ref=dst.at[t], send_sem=send.at[t], recv_sem=recv.at[t],
            device_id={"dp": to}, device_id_type=MESH)

    gq_copy.wait()
    head = FIRST * ROWS
    for s, (base, q) in enumerate(turns):
        a = base + q
        w_copy(s).wait()
        part[a, :head, :] = jnp.dot(
            gqv[:head, :], wv[a], preferred_element_type=F32).astype(BF16)
        if s == 0:
            @pl.when(is_inner)
            def _():
                pl.semaphore_wait(barrier, 5)

            @pl.when(is_outer)
            def _():
                pl.semaphore_wait(barrier, 4)

        if s % 2 == 1:
            @pl.when(is_outer)
            def _():
                for c in range(FIRST if s == 1 else FIRST - LEAD):
                    to_mate(part, from_mate, base, c).start()

    for a in range(QUARTERS):
        r_copy(a).start()
    for a in range(QUARTERS):
        gi_copy(a).start()

    for base, q in turns:
        a = base + q
        part[a, head:, :] = jnp.dot(
            gqv[head:, :], wv[a], preferred_element_type=F32).astype(BF16)

    @pl.when(is_outer)
    def _():
        @pl.loop(FIRST, chunks)
        def _(c):
            to_mate(part, from_mate, other, c).start()
            to_mate(part, from_mate, own, c - LEAD).start()

        for c in range(chunks - LEAD, chunks):
            to_mate(part, from_mate, own, c).start()

    gain_copy.wait()
    lanes = gain_v.shape[1]
    for g in range(width // lanes):
        a, at_lane = g * lanes // span, g * lanes % span
        gain_f[a, :, at_lane:at_lane + lanes] = gain_v[g:g + 1, :].astype(F32)
    for a in range(QUARTERS):
        r_copy(a).wait()
        gi_copy(a).wait()
    gacc[...] = jnp.zeros_like(gacc)

    def norm(c):
        r = rows_of(c)
        total = jnp.zeros((ROWS, span), F32)
        for a in range(QUARTERS):
            x = rv[a, r, :].astype(F32)
            total = total + x * x
        scale = lax.rsqrt(jnp.sum(total, axis=-1, keepdims=True) * (1.0 / width) + 1e-05)
        inv[r, :] = scale
        for a in range(QUARTERS):
            nv[a, r, :] = (rv[a, r, :].astype(F32) * scale * gain_f[a]).astype(BF16)

    def regroup():
        gq_t[...] = gqv[...].T
        for v in range(2):
            for j, rel in enumerate(((0, 2, 1, 3), (0, 1, 2, 3))[v]):
                y_to = yy + (rel // 2) * (1 - 2 * yy)
                x_to = xx + (rel % 2) * (1 - 2 * xx)
                for mine in range(2):
                    c_to = core if mine else 1 - core
                    at = pl.multiple_of((y_to * 4 + x_to * 2 + c_to) * block, block)
                    gq_p[v, mine, j * block:(j + 1) * block, :] = gq_t[pl.ds(at, block), :]

    first, second = (x_mate, y_mate), (y_mate, x_mate)

    def product(mine, j, v):
        return jnp.dot(gq_p[v, mine], nv[j, :, v * cols:(v + 1) * cols], preferred_element_type=F32)

    def stage1(j):
        for v in range(2):
            t = 2 * j + v
            fgs[t] = product(0, j, v).astype(BF16)
            hop(fgs, fgr, s1, r1, t, core_mate).start()

    def stage2(j):
        for v in range(2):
            t = 2 * j + v
            hop(fgs, fgr, s1, r1, t, core_mate).wait_recv()
            total = product(1, j, v) + fgr[t].astype(F32)
            xs[t] = total[2 * block:].astype(BF16)
            hop(xs, xr, s2, r2, t, first[v]).start()
            keep[t] = total[:2 * block]

    def stage3(j):
        for v in range(2):
            t = 2 * j + v
            hop(xs, xr, s2, r2, t, first[v]).wait_recv()
            ys[t] = (keep[t, block:] + xr[t, block:].astype(F32)).astype(BF16)
            hop(ys, yr, s3, r3, t, second[v]).start()
            keep[t, :block] = keep[t, :block] + xr[t, :block].astype(F32)

    def stage4(j):
        for v in range(2):
            t = 2 * j + v
            hop(ys, yr, s3, r3, t, second[v]).wait_recv()
            wgo[t] = keep[t, :block] + yr[t].astype(F32)

    def pass_on(c):
        r = rows_of(c)
        to_mate(part, from_mate, other, c).wait_recv()
        for q in range(2):
            a = other + q
            part[a, r, :] = (
                part[a, r, :].astype(F32) + from_mate[a, r, :].astype(F32)).astype(BF16)
        to_peer(part, from_peer, other, c).start()

    def root(c):
        r = rows_of(c)
        to_mate(part, from_mate, own, c).wait_recv()
        to_peer(part, from_peer, own, c).wait_recv()
        terms = []
        for q in range(2):
            a = own + q
            dnormed = part[a, r, :].astype(F32) + from_mate[a, r, :].astype(F32)
            dnormed = dnormed + from_peer[a, r, :].astype(F32)
            ds[a, r, :] = dnormed.astype(BF16)
            terms.append(dnormed * (rv[a, r, :].astype(F32) * inv[r, :]))
        to_mate(ds, ds, own, c).start()
        to_peer(ds, ds, own, c).start()
        for q in range(2):
            gacc[q] += terms[q][:8] + terms[q][8:]

    def forward(c):
        to_peer(ds, ds, other, c).wait_recv()
        to_mate(ds, ds, other, c).start()

    def collect(c):
        for base in (0, 2):
            to_mate(part, ds, base, c).wait_recv()

    def finish(c):
        r = rows_of(c)
        scale = inv[r, :]
        total = jnp.zeros((ROWS, span), F32)
        for a in range(QUARTERS):
            total = total + ds[a, r, :].astype(F32) * gain_f[a] * (rv[a, r, :].astype(F32) * scale)
        mean = jnp.sum(total, axis=-1, keepdims=True) * (1.0 / width)
        for a in range(QUARTERS):
            dunit = ds[a, r, :].astype(F32) * gain_f[a]
            unit = rv[a, r, :].astype(F32) * scale
            gov[a, r, :] = (
                giv[a, r, :].astype(F32) + scale * (dunit - unit * mean)).astype(BF16)

    def g_copy(o):
        return pltpu.make_async_remote_copy(
            src_ref=gslot.at[0], dst_ref=gslot.at[o], send_sem=sg.at[o], recv_sem=rg.at[o],
            device_id={"dp": (dp + o) % n_dp}, device_id_type=MESH)

    targets = (mate, peer, (1 - h) * (n_tp - 1))

    def z_copy(i):
        return pltpu.make_async_remote_copy(
            src_ref=gz.at[h], dst_ref=gz.at[h], send_sem=sz.at[i], recv_sem=rz.at[h],
            device_id={"tp": targets[i]}, device_id_type=MESH)

    def z_wait(which):
        pltpu.make_async_remote_copy(
            src_ref=gz.at[which], dst_ref=gz.at[which], send_sem=sz.at[0], recv_sem=rz.at[which],
            device_id={"tp": mate}, device_id_type=MESH).wait_recv()

    def at(i, lo, hi):
        return jnp.logical_and(i >= lo, i < hi)

    @pl.loop(0, chunks + LAG)
    def _(i):
        @pl.when(jnp.logical_and(is_inner, i < chunks))
        def _():
            pass_on(i)

        @pl.when(jnp.logical_and(is_inner, at(i, 4, chunks + 4)))
        def _():
            forward(i - 4)

        @pl.when(jnp.logical_and(is_inner, at(i, 2, chunks + 2)))
        def _():
            root(i - 2)

        @pl.when(jnp.logical_and(is_inner, i == chunks + 1))
        def _():
            for q in range(2):
                gslot[0, q:q + 1, :] = jnp.sum(gacc[q], axis=0, keepdims=True)
            for o in range(1, n_dp):
                g_copy(o).start()

        @pl.when(jnp.logical_and(is_inner, at(i, 5, chunks + 5)))
        def _():
            finish(i - 5)

        @pl.when(jnp.logical_and(is_outer, i >= LAG))
        def _():
            collect(i - LAG)
            finish(i - LAG)

        @pl.when(i == 0)
        def _():
            pl.loop(0, 9)(norm)

        @pl.when(i == 1)
        def _():
            pl.loop(9, 13)(norm)

        @pl.when(i == 2)
        def _():
            pl.loop(13, chunks)(norm)
            regroup()

        @pl.when(at(i, 3, 5))
        def _():
            stage1(2 * (i - 3))
            stage1(2 * (i - 3) + 1)

        @pl.when(at(i, 5, 9))
        def _():
            stage2(i - 5)

        @pl.when(at(i, 9, 13))
        def _():
            stage3(i - 9)

        @pl.when(at(i, 13, 17))
        def _():
            stage4(i - 13)

    @pl.when(is_inner)
    def _():
        for o in range(1, n_dp):
            g_copy(o).wait_recv()
        total = gslot[dp % n_dp]
        for d in range(1, n_dp):
            total = total + gslot[(dp + n_dp - d) % n_dp]
        gz[h] = total
        for i in range(3):
            z_copy(i).start()
        z_wait(1 - h)
        for i in range(3):
            z_copy(i).wait_send()
        for o in range(1, n_dp):
            g_copy(o).wait_send()
        pltpu.make_async_remote_copy(
            src_ref=part, dst_ref=ds, send_sem=sp.at[0], recv_sem=rp.at[0],
            device_id={"tp": peer}, device_id_type=MESH).wait_send()

    @pl.when(is_outer)
    def _():
        z_wait(0)
        z_wait(1)

    for a in range(QUARTERS):
        ggv[:, a * span:(a + 1) * span] = gz[a // 2, a % 2:a % 2 + 1, :]
    pltpu.make_async_remote_copy(
        src_ref=part, dst_ref=ds, send_sem=so.at[0], recv_sem=rm.at[0],
        device_id={"tp": mate}, device_id_type=MESH).wait_send()

    for t in range(TILES):
        hop(fgs, fgr, s1, r1, t, core_mate).wait_send()
        hop(xs, xr, s2, r2, t, first[t % 2]).wait_send()
        hop(ys, yr, s3, r3, t, second[t % 2]).wait_send()


def write_out(wgo, ggv, gov, wg_out, gg_out, go_out, sem):
    cols, span = wgo.shape[2], gov.shape[2]
    copies = [pltpu.make_async_copy(ggv, gg_out, sem.at[TILES + QUARTERS])]
    for a in range(QUARTERS):
        copies.append(pltpu.make_async_copy(
            gov.at[a], go_out.at[:, a * span:(a + 1) * span], sem.at[TILES + a]))
    for t in range(TILES):
        copies.append(pltpu.make_async_copy(
            wgo.at[t], wg_out.at[:, t * cols:(t + 1) * cols], sem.at[t]))
    for copy in copies:
        copy.start()
    for copy in copies:
        copy.wait()


def fused(n_dp, n_tp, resid, gain, grad_q, w_query, grad_in):
    tokens, width = resid.shape
    heads = grad_q.shape[1]
    chunks = tokens // ROWS
    block, cols, span = heads // n_dp, width // TILES, width // QUARTERS
    any_space = pl.BlockSpec(memory_space=pl.ANY)
    dma = lambda n: pltpu.SemaphoreType.DMA((n,))
    wide = lambda: pltpu.VMEM((QUARTERS, tokens, span), BF16)
    vmem = pl.BlockSpec(memory_space=pltpu.VMEM)
    held = pl.pallas_call(
        functools.partial(kernel, n_dp, n_tp),
        out_shape=(
            pltpu.VMEM((TILES, block, cols), F32),
            pltpu.VMEM((1, width), F32),
            pltpu.VMEM((QUARTERS, tokens, span), BF16),
        ),
        in_specs=[any_space] * 5,
        out_specs=(vmem,) * 3,
        scratch_shapes=[
            pltpu.VMEM((QUARTERS, heads, span), BF16),
            wide(),
            pltpu.VMEM((tokens, heads), BF16),
            wide(), wide(), wide(), wide(), wide(), wide(),
            pltpu.VMEM((width // 128, 128), BF16),
            pltpu.VMEM((QUARTERS, 1, span), F32),
            pltpu.VMEM((tokens, 1), F32),
            pltpu.VMEM((heads, tokens), BF16),
            pltpu.VMEM((2, 2, 4 * block, tokens), BF16),
            pltpu.VMEM((TILES, 4 * block, cols), BF16),
            pltpu.VMEM((TILES, 4 * block, cols), BF16),
            pltpu.VMEM((TILES, 2 * block, cols), F32),
            pltpu.VMEM((TILES, 2 * block, cols), BF16),
            pltpu.VMEM((TILES, 2 * block, cols), BF16),
            pltpu.VMEM((TILES, block, cols), BF16),
            pltpu.VMEM((TILES, block, cols), BF16),
            pltpu.VMEM((2, 8, span), F32),
            pltpu.VMEM((n_dp, 2, span), F32),
            pltpu.VMEM((2, 2, span), F32),
            dma(QUARTERS), dma(3), dma(QUARTERS), dma(QUARTERS), dma(1), dma(1),
            dma(2 * chunks), dma(2 * chunks),
            dma(TILES), dma(TILES), dma(TILES), dma(TILES), dma(TILES), dma(TILES),
            dma(n_dp), dma(n_dp), dma(3), dma(2),
        ],
        compiler_params=pltpu.CompilerParams(
            collective_id=0, has_side_effects=True, vmem_limit_bytes=VMEM_MIB * 1024 * 1024
        ),
    )(resid, gain.reshape(width // 128, 128), grad_q, w_query, grad_in)
    weight_grad, gain_grad, grad_rows = pl.pallas_call(
        write_out,
        out_shape=(
            jax.ShapeDtypeStruct((block, width), F32),
            jax.ShapeDtypeStruct((1, width), F32),
            jax.ShapeDtypeStruct((tokens, width), BF16),
        ),
        in_specs=[vmem] * 3,
        out_specs=(any_space,) * 3,
        scratch_shapes=[dma(TILES + QUARTERS + 1)],
        compiler_params=pltpu.CompilerParams(vmem_limit_bytes=1024 * 1024),
    )(*held)
    return weight_grad, gain_grad.reshape(width), grad_rows


def solution(mesh):
    n_dp, n_tp = mesh.shape["dp"], mesh.shape["tp"]
    if (n_dp, n_tp) == (2 * 2 * 2, 4):
        body = functools.partial(fused, n_dp, n_tp)
    else:
        body = per_device
    return jax.shard_map(
        body,
        mesh=mesh,
        in_specs=(P("dp", None), P(), P("dp", "tp"), P("tp", None), P("dp", None)),
        out_specs=(P(("tp", "dp"), None), P(), P("dp", None)),
        check_vma=False,
    )
```

```python
import functools

import jax
import jax.numpy as jnp
from jax import lax
from jax.experimental import pallas as pl
from jax.experimental.pallas import tpu as pltpu
from jax.sharding import PartitionSpec as P

MESH = pl.DeviceIdType.MESH
F32 = jnp.float32
BF16 = jnp.bfloat16
ROWS = 16
TILES = 8
QUARTERS = 4
LEAD = 2
FIRST = LEAD + 1
VMEM_MIB = 52
LAG = 6
MIDDLE = 8


def norm_rows(rows_bf, gain_f):
    rows_f = rows_bf.astype(jnp.float32)
    inv_rms = lax.rsqrt(jnp.mean(rows_f * rows_f, axis=-1, keepdims=True) + 1e-05)
    unit = rows_f * inv_rms
    return (inv_rms, unit, (unit * gain_f).astype(jnp.bfloat16))


def per_device(resid, gain, grad_q, w_query, grad_in):
    gain_f = gain.astype(jnp.float32)
    inv_rms, unit, normed = norm_rows(resid, gain_f)
    local_term = jnp.dot(grad_q, w_query, preferred_element_type=jnp.float32)
    dnormed = lax.psum(local_term.astype(jnp.bfloat16), "tp").astype(jnp.float32)
    full_grad = lax.dot_general(
        grad_q, normed, (((0,), (0,)), ((), ())), preferred_element_type=jnp.float32
    )
    weight_grad = lax.psum_scatter(full_grad, "dp", scatter_dimension=0, tiled=True)
    gain_grad = lax.psum(jnp.sum(dnormed * unit, axis=0), "dp")
    dunit = dnormed * gain_f
    inner = jnp.mean(dunit * unit, axis=-1, keepdims=True)
    grad_rows = (grad_in.astype(jnp.float32) + inv_rms * (dunit - unit * inner)).astype(
        jnp.bfloat16
    )
    return (weight_grad, gain_grad, grad_rows)


def residual_rows(summed, rows, above, scale, gain_f, out, at):
    span = gain_f.shape[2]
    total = jnp.zeros((ROWS, span), F32)
    for a in range(QUARTERS):
        total = total + summed(a).astype(F32) * gain_f[a] * (rows(a).astype(F32) * scale)
    mean = jnp.sum(total, axis=-1, keepdims=True) * (1.0 / (QUARTERS * span))
    for a in range(QUARTERS):
        dunit = summed(a).astype(F32) * gain_f[a]
        unit = rows(a).astype(F32) * scale
        out[a, at, :] = (above(a).astype(F32) + scale * (dunit - unit * mean)).astype(BF16)


def kernel(n_dp, n_tp, resid, gain, grad_q, w_query, grad_in, wgo, ggv, gov, ds_end, rv_end, gi_end, inv_end, gain_f,
           wv, rv, gqv, giv, nv, part, from_mate, from_peer, ds, gain_v, inv, gq_t, gq_p,
           fgs, fgr, keep, xs, xr, ys, yr, gacc, gslot, gz,
           gqx, w_sem, in_sem, r_sem, gi_sem, so, sp, rm, rp, sq, rq, sx, rx,
           s1, r1, s2, r2, s3, r3, sg, rg, sz, rz):
    dp, tp = lax.axis_index("dp"), lax.axis_index("tp")
    _, tokens, span = rv.shape
    heads = gqv.shape[1]
    width = QUARTERS * span
    chunks = tokens // ROWS
    cols = width // TILES
    block = heads // n_dp
    h = tp // 2
    is_inner = jnp.logical_and(tp > 0, tp < n_tp - 1)
    is_outer = jnp.logical_not(is_inner)
    mate = jnp.where(is_inner, h * (n_tp - 1), 1 + h)
    peer = 2 - h
    core, xx, yy = dp % 2, (dp // 2) % 2, dp // 4
    core_mate = dp + 1 - 2 * core
    x_mate = dp + 2 - 4 * xx
    y_mate = dp + 4 - 8 * yy
    own, other = h, 1 - h
    last = chunks - 1
    count = last + 2 * core

    def nth(k):
        moved = jnp.where(k < MIDDLE, k, jnp.where(k == MIDDLE, chunks, k - 1))
        return jnp.where(core == 1, moved, k)

    turns = ((other, 0), (other, 1), (own, 0), (own, 1))

    def span_of(a):
        return pl.ds(pl.multiple_of(a * span, span), span)

    def lanes_of(q):
        return slice(q * span, (q + 1) * span)

    def w_copy(s):
        a = 2 * turns[s][0] + turns[s][1]
        return pltpu.make_async_copy(w_query.at[:, span_of(a)], wv.at[a], w_sem.at[s])

    def r_copy(a):
        return pltpu.make_async_copy(
            resid.at[:, a * span:(a + 1) * span], rv.at[a], r_sem.at[a])

    def gi_copy(a):
        return pltpu.make_async_copy(
            grad_in.at[:, a * span:(a + 1) * span], giv.at[a], gi_sem.at[a])

    gq_copy = pltpu.make_async_copy(grad_q, gqv, in_sem.at[0])
    gain_copy = pltpu.make_async_copy(gain, gain_v, in_sem.at[1])
    gq_copy.start()
    gain_copy.start()
    for s in range(QUARTERS):
        w_copy(s).start()

    barrier = pltpu.get_barrier_semaphore()
    for to in (core_mate, x_mate, y_mate):
        pl.semaphore_signal(barrier, inc=1, device_id={"dp": to}, device_id_type=MESH)
    pl.semaphore_signal(barrier, inc=1, device_id={"tp": mate}, device_id_type=MESH)

    @pl.when(is_inner)
    def _():
        pl.semaphore_signal(barrier, inc=1, device_id={"tp": peer}, device_id_type=MESH)

    def rows_of(c):
        return pl.ds(pl.multiple_of(c * ROWS, ROWS), ROWS)

    def to_mate(src, dst, half, c):
        return pltpu.make_async_remote_copy(
            src_ref=src.at[half, rows_of(c)], dst_ref=dst.at[half, rows_of(c)],
            send_sem=so.at[0], recv_sem=rm.at[2 * c + half],
            device_id={"tp": mate}, device_id_type=MESH)

    def to_peer(src, dst, half, c):
        return pltpu.make_async_remote_copy(
            src_ref=src.at[half, rows_of(c)], dst_ref=dst.at[half, rows_of(c)],
            send_sem=sp.at[0], recv_sem=rp.at[2 * c + half],
            device_id={"tp": peer}, device_id_type=MESH)

    def hop(src, dst, send, recv, t, to):
        return pltpu.make_async_remote_copy(
            src_ref=src.at[t], dst_ref=dst.at[t], send_sem=send.at[t], recv_sem=recv.at[t],
            device_id={"dp": to}, device_id_type=MESH)

    gq_copy.wait()
    head = FIRST * ROWS
    for s, (base, q) in enumerate(turns):
        w_copy(s).wait()
        part[base, :head, lanes_of(q)] = jnp.dot(
            gqv[:head, :], wv[2 * base + q], preferred_element_type=F32).astype(BF16)
        if s == 1:
            @pl.when(is_inner)
            def _():
                pl.semaphore_wait(barrier, 5)

            @pl.when(is_outer)
            def _():
                pl.semaphore_wait(barrier, 4)

        if s % 2 == 1:
            @pl.when(is_outer)
            def _():
                for c in range(FIRST if s == 1 else FIRST - LEAD):
                    to_mate(part, from_mate, base, c).start()

    ends = pltpu.make_async_remote_copy(
        src_ref=gqv.at[tokens - ROWS:], dst_ref=gqx, send_sem=sq.at[0], recv_sem=rq.at[0],
        device_id={"dp": core_mate}, device_id_type=MESH)
    pl.when(core == 0)(ends.start)
    for a in range(QUARTERS):
        r_copy(a).start()
    for a in range(QUARTERS):
        gi_copy(a).start()

    for base, q in turns:
        part[base, head:tokens, lanes_of(q)] = jnp.dot(
            gqv[head:, :], wv[2 * base + q], preferred_element_type=F32).astype(BF16)

    @pl.when(core == 1)
    def _():
        ends.wait_recv()
        for base, q in turns:
            part[base, tokens:, lanes_of(q)] = jnp.dot(
                gqx[...], wv[2 * base + q], preferred_element_type=F32).astype(BF16)

    @pl.when(is_outer)
    def _():
        @pl.loop(FIRST, count)
        def _(k):
            to_mate(part, from_mate, other, nth(k)).start()
            to_mate(part, from_mate, own, nth(k - LEAD)).start()

        for j in range(LEAD):
            to_mate(part, from_mate, own, nth(count - LEAD + j)).start()

    gain_copy.wait()
    lanes = gain_v.shape[1]
    for g in range(width // lanes):
        a, at_lane = g * lanes // span, g * lanes % span
        gain_f[a, :, at_lane:at_lane + lanes] = gain_v[g:g + 1, :].astype(F32)
    for a in range(QUARTERS):
        r_copy(a).wait()
        gi_copy(a).wait()
    gacc[...] = jnp.zeros_like(gacc)

    def norm(c):
        r = rows_of(c)
        total = jnp.zeros((ROWS, span), F32)
        for a in range(QUARTERS):
            x = rv[a, r, :].astype(F32)
            total = total + x * x
        scale = lax.rsqrt(jnp.sum(total, axis=-1, keepdims=True) * (1.0 / width) + 1e-05)
        inv[r, :] = scale
        for a in range(QUARTERS):
            nv[a, r, :] = (rv[a, r, :].astype(F32) * scale * gain_f[a]).astype(BF16)

    def regroup():
        gq_t[...] = gqv[...].T
        for v in range(2):
            for j, rel in enumerate(((0, 2, 1, 3), (0, 1, 2, 3))[v]):
                y_to = yy + (rel // 2) * (1 - 2 * yy)
                x_to = xx + (rel % 2) * (1 - 2 * xx)
                for mine in range(2):
                    c_to = core if mine else 1 - core
                    at = pl.multiple_of((y_to * 4 + x_to * 2 + c_to) * block, block)
                    gq_p[v, mine, j * block:(j + 1) * block, :] = gq_t[pl.ds(at, block), :]

    first, second = (x_mate, y_mate), (y_mate, x_mate)

    def product(mine, j, v):
        return jnp.dot(gq_p[v, mine], nv[j, :, v * cols:(v + 1) * cols], preferred_element_type=F32)

    def stage1(j):
        for v in range(2):
            t = 2 * j + v
            fgs[t] = product(0, j, v).astype(BF16)
            hop(fgs, fgr, s1, r1, t, core_mate).start()

    def stage2(j):
        for v in range(2):
            t = 2 * j + v
            hop(fgs, fgr, s1, r1, t, core_mate).wait_recv()
            total = product(1, j, v) + fgr[t].astype(F32)
            xs[t] = total[2 * block:].astype(BF16)
            hop(xs, xr, s2, r2, t, first[v]).start()
            keep[t] = total[:2 * block]

    def stage3(j):
        for v in range(2):
            t = 2 * j + v
            hop(xs, xr, s2, r2, t, first[v]).wait_recv()
            ys[t] = (keep[t, block:] + xr[t, block:].astype(F32)).astype(BF16)
            hop(ys, yr, s3, r3, t, second[v]).start()
            keep[t, :block] = keep[t, :block] + xr[t, :block].astype(F32)

    def stage4(j):
        for v in range(2):
            t = 2 * j + v
            hop(ys, yr, s3, r3, t, second[v]).wait_recv()
            wgo[t] = keep[t, :block] + yr[t].astype(F32)

    def pass_on(c):
        r = rows_of(c)
        to_mate(part, from_mate, other, c).wait_recv()
        for q in range(2):
            at = (other, r, lanes_of(q))
            part[at] = (part[at].astype(F32) + from_mate[at].astype(F32)).astype(BF16)
        to_peer(part, from_peer, other, c).start()

    def root(c):
        r = rows_of(c)
        to_mate(part, from_mate, own, c).wait_recv()
        to_peer(part, from_peer, own, c).wait_recv()
        mine = jnp.minimum(c, last)
        keep_it = jnp.where(c == chunks, 0.0, 1.0)
        terms = []
        for q in range(2):
            at = (own, r, lanes_of(q))
            dnormed = part[at].astype(F32) + from_mate[at].astype(F32)
            dnormed = dnormed + from_peer[at].astype(F32)
            ds[at] = dnormed.astype(BF16)
            unit = rv[2 * own + q, rows_of(mine), :].astype(F32) * inv[rows_of(mine), :]
            terms.append(dnormed * unit * keep_it)
        to_mate(ds, ds, own, c).start()
        to_peer(ds, ds, own, c).start()
        for q in range(2):
            gacc[q] += terms[q][:8] + terms[q][8:]

    def forward(c):
        to_peer(ds, ds, other, c).wait_recv()
        to_mate(ds, ds, other, c).start()

    def give(half):
        return pltpu.make_async_remote_copy(
            src_ref=ds.at[half, rows_of(chunks)], dst_ref=ds.at[half, rows_of(last)],
            send_sem=sx.at[half], recv_sem=rx.at[half],
            device_id={"dp": core_mate}, device_id_type=MESH)

    def give_both():
        for half in range(2):
            give(half).start()

    def absorb():
        give(own).wait_recv()
        r = rows_of(last)
        for q in range(2):
            unit = rv[2 * own + q, r, :].astype(F32) * inv[r, :]
            term = ds[own, r, lanes_of(q)].astype(F32) * unit
            gacc[q] += term[:8] + term[8:]

    def collect(c):
        for half in range(2):
            to_mate(part, ds, half, c).wait_recv()

    def finish(c):
        r = rows_of(c)
        residual_rows(
            lambda a: ds[a // 2, r, lanes_of(a % 2)], lambda a: rv[a, r, :],
            lambda a: giv[a, r, :], inv[r, :], gain_f, gov, r)

    def g_copy(o):
        return pltpu.make_async_remote_copy(
            src_ref=gslot.at[0], dst_ref=gslot.at[o], send_sem=sg.at[o], recv_sem=rg.at[o],
            device_id={"dp": (dp + o) % n_dp}, device_id_type=MESH)

    targets = (mate, peer, (1 - h) * (n_tp - 1))

    def z_copy(i):
        return pltpu.make_async_remote_copy(
            src_ref=gz.at[h], dst_ref=gz.at[h], send_sem=sz.at[i], recv_sem=rz.at[h],
            device_id={"tp": targets[i]}, device_id_type=MESH)

    def z_wait(which):
        pltpu.make_async_remote_copy(
            src_ref=gz.at[which], dst_ref=gz.at[which], send_sem=sz.at[0], recv_sem=rz.at[which],
            device_id={"tp": mate}, device_id_type=MESH).wait_recv()

    def sent(sem):
        for which, rows in ((0, tokens - ROWS), (1, tokens + ROWS)):
            @pl.when(core == which)
            def _():
                pltpu.make_async_remote_copy(
                    src_ref=part.at[:, :rows], dst_ref=ds.at[:, :rows], send_sem=sem.at[0],
                    recv_sem=rm.at[0], device_id={"tp": mate}, device_id_type=MESH).wait_send()

    def at(i, lo, hi):
        return jnp.logical_and(i >= lo, i < hi)

    extra = jnp.logical_and(core == 1, is_inner)

    @pl.loop(0, chunks + LAG)
    def _(i):
        @pl.when(jnp.logical_and(is_inner, i < count))
        def _():
            pass_on(nth(i))

        @pl.when(jnp.logical_and(is_inner, at(i, 4, count + 4)))
        def _():
            forward(nth(i - 4))

        @pl.when(jnp.logical_and(extra, i == MIDDLE + 4))
        def _():
            give_both()

        @pl.when(jnp.logical_and(jnp.logical_and(is_inner, core == 0), i == chunks - 1))
        def _():
            absorb()

        @pl.when(jnp.logical_and(is_inner, at(i, 2, count + 2)))
        def _():
            root(nth(i - 2))

        @pl.when(jnp.logical_and(is_inner, i == count + 1))
        def _():
            for q in range(2):
                gslot[0, q:q + 1, :] = jnp.sum(gacc[q], axis=0, keepdims=True)
            for o in range(1, n_dp):
                g_copy(o).start()

        @pl.when(jnp.logical_and(is_inner, at(i, 5, count + 5)))
        def _():
            pl.when(nth(i - 5) < last)(lambda: finish(nth(i - 5)))

        @pl.when(jnp.logical_and(is_outer, at(i, LAG, last + core + LAG)))
        def _():
            collect(nth(i - LAG))
            pl.when(nth(i - LAG) < last)(lambda: finish(nth(i - LAG)))
            pl.when(nth(i - LAG) == chunks)(give_both)

        @pl.when(i == 0)
        def _():
            pl.loop(0, 9)(norm)

        @pl.when(i == 1)
        def _():
            pl.loop(9, 13)(norm)

        @pl.when(i == 3)
        def _():
            rv_end[...] = rv[:, tokens - ROWS:, :]
            gi_end[...] = giv[:, tokens - ROWS:, :]
            inv_end[...] = inv[tokens - ROWS:, :]

        @pl.when(i == 2)
        def _():
            pl.loop(13, chunks)(norm)
            regroup()

        @pl.when(at(i, 3, 5))
        def _():
            stage1(2 * (i - 3))
            stage1(2 * (i - 3) + 1)

        @pl.when(at(i, 5, 9))
        def _():
            stage2(i - 5)

        @pl.when(at(i, 9, 13))
        def _():
            stage3(i - 9)

        @pl.when(at(i, 13, 17))
        def _():
            stage4(i - 13)

    @pl.when(is_inner)
    def _():
        for o in range(1, n_dp):
            g_copy(o).wait_recv()
        total = gslot[dp % n_dp]
        for d in range(1, n_dp):
            total = total + gslot[(dp + n_dp - d) % n_dp]
        gz[h] = total
        for i in range(3):
            z_copy(i).start()
        z_wait(1 - h)
        for i in range(3):
            z_copy(i).wait_send()
        for o in range(1, n_dp):
            g_copy(o).wait_send()
        sent(sp)

    pl.when(jnp.logical_and(is_outer, core == 1))(lambda: collect(last))

    @pl.when(core == 0)
    def _():
        ends.wait_send()
        pl.when(is_outer)(lambda: give(own).wait_recv())
        give(other).wait_recv()

    @pl.when(core == 1)
    def _():
        for half in range(2):
            give(half).wait_send()

    ds_end[...] = ds[:, tokens - ROWS:tokens, :]

    @pl.when(is_outer)
    def _():
        z_wait(0)
        z_wait(1)

    for a in range(QUARTERS):
        ggv[:, a * span:(a + 1) * span] = gz[a // 2, a % 2:a % 2 + 1, :]
    sent(so)

    for t in range(TILES):
        hop(fgs, fgr, s1, r1, t, core_mate).wait_send()
        hop(xs, xr, s2, r2, t, first[t % 2]).wait_send()
        hop(ys, yr, s3, r3, t, second[t % 2]).wait_send()


def write_out(wgo, ggv, gov, ds_end, rv_end, gi_end, inv_end, gain_f,
              wg_out, gg_out, go_out, end, sem):
    cols, span = wgo.shape[2], gov.shape[2]
    done = gov.shape[1] - ROWS
    copies = [
        pltpu.make_async_copy(
            gov.at[a, :done], go_out.at[:done, a * span:(a + 1) * span], sem.at[a])
        for a in range(QUARTERS)
    ]
    copies += [
        pltpu.make_async_copy(
            wgo.at[t], wg_out.at[:, t * cols:(t + 1) * cols], sem.at[QUARTERS + t])
        for t in range(TILES)
    ]
    copies.append(pltpu.make_async_copy(ggv, gg_out, sem.at[QUARTERS + TILES]))
    for copy in copies:
        copy.start()
    residual_rows(
        lambda a: ds_end[a // 2, :, a % 2 * span:(a % 2 + 1) * span], lambda a: rv_end[a],
        lambda a: gi_end[a], inv_end[...], gain_f, end, slice(0, ROWS))
    for a in range(QUARTERS):
        copies.append(pltpu.make_async_copy(
            end.at[a], go_out.at[done:, a * span:(a + 1) * span],
            sem.at[QUARTERS + TILES + 1 + a]))
        copies[-1].start()
    for copy in copies:
        copy.wait()


def fused(n_dp, n_tp, resid, gain, grad_q, w_query, grad_in):
    tokens, width = resid.shape
    heads = grad_q.shape[1]
    chunks = tokens // ROWS
    block, cols, span = heads // n_dp, width // TILES, width // QUARTERS
    any_space = pl.BlockSpec(memory_space=pl.ANY)
    dma = lambda n: pltpu.SemaphoreType.DMA((n,))
    wide = lambda: pltpu.VMEM((QUARTERS, tokens, span), BF16)
    halves = lambda: pltpu.VMEM((2, tokens + ROWS, 2 * span), BF16)
    vmem = pl.BlockSpec(memory_space=pltpu.VMEM)
    held = pl.pallas_call(
        functools.partial(kernel, n_dp, n_tp),
        out_shape=(
            pltpu.VMEM((TILES, block, cols), F32),
            pltpu.VMEM((1, width), F32),
            pltpu.VMEM((QUARTERS, tokens, span), BF16),
            pltpu.VMEM((2, ROWS, 2 * span), BF16),
            pltpu.VMEM((QUARTERS, ROWS, span), BF16),
            pltpu.VMEM((QUARTERS, ROWS, span), BF16),
            pltpu.VMEM((ROWS, 1), F32),
            pltpu.VMEM((QUARTERS, 1, span), F32),
        ),
        in_specs=[any_space] * 5,
        out_specs=(vmem,) * 8,
        scratch_shapes=[
            pltpu.VMEM((QUARTERS, heads, span), BF16),
            wide(),
            pltpu.VMEM((tokens, heads), BF16),
            wide(), wide(), halves(), halves(), halves(), halves(),
            pltpu.VMEM((width // 128, 128), BF16),
            pltpu.VMEM((tokens, 1), F32),
            pltpu.VMEM((heads, tokens), BF16),
            pltpu.VMEM((2, 2, 4 * block, tokens), BF16),
            pltpu.VMEM((TILES, 4 * block, cols), BF16),
            pltpu.VMEM((TILES, 4 * block, cols), BF16),
            pltpu.VMEM((TILES, 2 * block, cols), F32),
            pltpu.VMEM((TILES, 2 * block, cols), BF16),
            pltpu.VMEM((TILES, 2 * block, cols), BF16),
            pltpu.VMEM((TILES, block, cols), BF16),
            pltpu.VMEM((TILES, block, cols), BF16),
            pltpu.VMEM((2, 8, span), F32),
            pltpu.VMEM((n_dp, 2, span), F32),
            pltpu.VMEM((2, 2, span), F32),
            pltpu.VMEM((ROWS, heads), BF16),
            dma(QUARTERS), dma(3), dma(QUARTERS), dma(QUARTERS), dma(1), dma(1),
            dma(2 * chunks + 2), dma(2 * chunks + 2), dma(1), dma(1), dma(2), dma(2),
            dma(TILES), dma(TILES), dma(TILES), dma(TILES), dma(TILES), dma(TILES),
            dma(n_dp), dma(n_dp), dma(3), dma(2),
        ],
        compiler_params=pltpu.CompilerParams(
            collective_id=0, has_side_effects=True, vmem_limit_bytes=VMEM_MIB * 1024 * 1024
        ),
    )(resid, gain.reshape(width // 128, 128), grad_q, w_query, grad_in)
    weight_grad, gain_grad, grad_rows = pl.pallas_call(
        write_out,
        out_shape=(
            jax.ShapeDtypeStruct((block, width), F32),
            jax.ShapeDtypeStruct((1, width), F32),
            jax.ShapeDtypeStruct((tokens, width), BF16),
        ),
        in_specs=[vmem] * 8,
        out_specs=(any_space,) * 3,
        scratch_shapes=[
            pltpu.VMEM((QUARTERS, ROWS, span), BF16), dma(TILES + 2 * QUARTERS + 1)],
        compiler_params=pltpu.CompilerParams(vmem_limit_bytes=2 * 1024 * 1024),
    )(*held)
    return weight_grad, gain_grad.reshape(width), grad_rows


def solution(mesh):
    n_dp, n_tp = mesh.shape["dp"], mesh.shape["tp"]
    if (n_dp, n_tp) == (2 * 2 * 2, 4):
        body = functools.partial(fused, n_dp, n_tp)
    else:
        body = per_device
    return jax.shard_map(
        body,
        mesh=mesh,
        in_specs=(P("dp", None), P(), P("dp", "tp"), P("tp", None), P("dp", None)),
        out_specs=(P(("tp", "dp"), None), P(), P("dp", None)),
        check_vma=False,
    )
```

```python
import functools

import jax
import jax.numpy as jnp
from jax import lax
from jax.experimental import pallas as pl
from jax.experimental.pallas import tpu as pltpu
from jax.sharding import PartitionSpec as P

MESH = pl.DeviceIdType.MESH
F32 = jnp.float32
BF16 = jnp.bfloat16
ROWS = 16
TILES = 8
QUARTERS = 4
LEAD = 2
FIRST = LEAD + 1
VMEM_MIB = 52
LAG = 6
MIDDLE = 8


def norm_rows(rows_bf, gain_f):
    rows_f = rows_bf.astype(jnp.float32)
    inv_rms = lax.rsqrt(jnp.mean(rows_f * rows_f, axis=-1, keepdims=True) + 1e-05)
    unit = rows_f * inv_rms
    return (inv_rms, unit, (unit * gain_f).astype(jnp.bfloat16))


def per_device(resid, gain, grad_q, w_query, grad_in):
    gain_f = gain.astype(jnp.float32)
    inv_rms, unit, normed = norm_rows(resid, gain_f)
    local_term = jnp.dot(grad_q, w_query, preferred_element_type=jnp.float32)
    dnormed = lax.psum(local_term.astype(jnp.bfloat16), "tp").astype(jnp.float32)
    full_grad = lax.dot_general(
        grad_q, normed, (((0,), (0,)), ((), ())), preferred_element_type=jnp.float32
    )
    weight_grad = lax.psum_scatter(full_grad, "dp", scatter_dimension=0, tiled=True)
    gain_grad = lax.psum(jnp.sum(dnormed * unit, axis=0), "dp")
    dunit = dnormed * gain_f
    inner = jnp.mean(dunit * unit, axis=-1, keepdims=True)
    grad_rows = (grad_in.astype(jnp.float32) + inv_rms * (dunit - unit * inner)).astype(
        jnp.bfloat16
    )
    return (weight_grad, gain_grad, grad_rows)


def residual_rows(summed, rows, above, scale, gain_f, out, at):
    span = gain_f.shape[2]
    total = jnp.zeros((ROWS, span), F32)
    for a in range(QUARTERS):
        total = total + summed(a).astype(F32) * gain_f[a] * (rows(a).astype(F32) * scale)
    mean = jnp.sum(total, axis=-1, keepdims=True) * (1.0 / (QUARTERS * span))
    for a in range(QUARTERS):
        dunit = summed(a).astype(F32) * gain_f[a]
        unit = rows(a).astype(F32) * scale
        out[a, at, :] = (above(a).astype(F32) + scale * (dunit - unit * mean)).astype(BF16)


def kernel(n_dp, n_tp, resid, gain, grad_q, w_query, grad_in, wgo, ggv, gov, ds_end, rv_end, gi_end, inv_end, gain_f,
           wv, rv, gqv, giv, nv, part, from_mate, from_peer, ds, gain_v, inv, gq_t, gq_p,
           fgs, fgr, keep, xs, xr, ys, yr, gacc, gslot, gz,
           gqx, w_sem, in_sem, r_sem, gi_sem, so, sp, rm, rp, sq, rq, sx, rx,
           s1, r1, s2, r2, s3, r3, sg, rg, sz, rz):
    dp, tp = lax.axis_index("dp"), lax.axis_index("tp")
    _, tokens, span = rv.shape
    heads = gqv.shape[1]
    width = QUARTERS * span
    chunks = tokens // ROWS
    cols = width // TILES
    block = heads // n_dp
    h = tp // 2
    is_inner = jnp.logical_and(tp > 0, tp < n_tp - 1)
    is_outer = jnp.logical_not(is_inner)
    mate = jnp.where(is_inner, h * (n_tp - 1), 1 + h)
    peer = 2 - h
    core, xx, yy = dp % 2, (dp // 2) % 2, dp // 4
    core_mate = dp + 1 - 2 * core
    x_mate = dp + 2 - 4 * xx
    y_mate = dp + 4 - 8 * yy
    own, other = h, 1 - h
    last = chunks - 1
    count = last + 2 * core

    def nth(k):
        moved = jnp.where(k < MIDDLE, k, jnp.where(k == MIDDLE, chunks, k - 1))
        return jnp.where(core == 1, moved, k)

    turns = ((other, 0), (other, 1), (own, 0), (own, 1))

    def span_of(a):
        return pl.ds(pl.multiple_of(a * span, span), span)

    def lanes_of(q):
        return slice(q * span, (q + 1) * span)

    def w_copy(s):
        a = 2 * turns[s][0] + turns[s][1]
        return pltpu.make_async_copy(w_query.at[:, span_of(a)], wv.at[a], w_sem.at[s])

    def r_copy(a):
        return pltpu.make_async_copy(
            resid.at[:, a * span:(a + 1) * span], rv.at[a], r_sem.at[a])

    def gi_copy(a):
        return pltpu.make_async_copy(
            grad_in.at[:, a * span:(a + 1) * span], giv.at[a], gi_sem.at[a])

    gq_copy = pltpu.make_async_copy(grad_q, gqv, in_sem.at[0])
    gain_copy = pltpu.make_async_copy(gain, gain_v, in_sem.at[1])
    gq_copy.start()
    gain_copy.start()
    for s in range(QUARTERS):
        w_copy(s).start()

    barrier = pltpu.get_barrier_semaphore()
    for to in (core_mate, x_mate, y_mate):
        pl.semaphore_signal(barrier, inc=1, device_id={"dp": to}, device_id_type=MESH)
    pl.semaphore_signal(barrier, inc=1, device_id={"tp": mate}, device_id_type=MESH)

    @pl.when(is_inner)
    def _():
        pl.semaphore_signal(barrier, inc=1, device_id={"tp": peer}, device_id_type=MESH)

    def rows_of(c):
        return pl.ds(pl.multiple_of(c * ROWS, ROWS), ROWS)

    def to_mate(src, dst, half, c):
        return pltpu.make_async_remote_copy(
            src_ref=src.at[half, rows_of(c)], dst_ref=dst.at[half, rows_of(c)],
            send_sem=so.at[0], recv_sem=rm.at[2 * c + half],
            device_id={"tp": mate}, device_id_type=MESH)

    def to_peer(src, dst, half, c):
        return pltpu.make_async_remote_copy(
            src_ref=src.at[half, rows_of(c)], dst_ref=dst.at[half, rows_of(c)],
            send_sem=sp.at[0], recv_sem=rp.at[2 * c + half],
            device_id={"tp": peer}, device_id_type=MESH)

    def hop(src, dst, send, recv, t, to):
        return pltpu.make_async_remote_copy(
            src_ref=src.at[t], dst_ref=dst.at[t], send_sem=send.at[t], recv_sem=recv.at[t],
            device_id={"dp": to}, device_id_type=MESH)

    gq_copy.wait()
    head = FIRST * ROWS
    for s, (base, q) in enumerate(turns):
        w_copy(s).wait()
        part[base, :head, lanes_of(q)] = jnp.dot(
            gqv[:head, :], wv[2 * base + q], preferred_element_type=F32).astype(BF16)
        if s == 1:
            @pl.when(is_inner)
            def _():
                pl.semaphore_wait(barrier, 5)

            @pl.when(is_outer)
            def _():
                pl.semaphore_wait(barrier, 4)

        if s % 2 == 1:
            @pl.when(is_outer)
            def _():
                for c in range(FIRST if s == 1 else FIRST - LEAD):
                    to_mate(part, from_mate, base, c).start()

    ends = pltpu.make_async_remote_copy(
        src_ref=gqv.at[tokens - ROWS:], dst_ref=gqx, send_sem=sq.at[0], recv_sem=rq.at[0],
        device_id={"dp": core_mate}, device_id_type=MESH)
    pl.when(core == 0)(ends.start)
    for a in range(QUARTERS):
        r_copy(a).start()
    for a in range(QUARTERS):
        gi_copy(a).start()

    for base, q in turns:
        part[base, head:tokens, lanes_of(q)] = jnp.dot(
            gqv[head:, :], wv[2 * base + q], preferred_element_type=F32).astype(BF16)

    @pl.when(core == 1)
    def _():
        ends.wait_recv()
        for base, q in turns:
            part[base, tokens:, lanes_of(q)] = jnp.dot(
                gqx[...], wv[2 * base + q], preferred_element_type=F32).astype(BF16)

    @pl.when(is_outer)
    def _():
        @pl.loop(FIRST, count)
        def _(k):
            to_mate(part, from_mate, other, nth(k)).start()
            to_mate(part, from_mate, own, nth(k - LEAD)).start()

        for j in range(LEAD):
            to_mate(part, from_mate, own, nth(count - LEAD + j)).start()

    gain_copy.wait()
    lanes = gain_v.shape[1]
    for g in range(width // lanes):
        a, at_lane = g * lanes // span, g * lanes % span
        gain_f[a, :, at_lane:at_lane + lanes] = gain_v[g:g + 1, :].astype(F32)
    for a in range(QUARTERS):
        r_copy(a).wait()
        gi_copy(a).wait()
    gacc[...] = jnp.zeros_like(gacc)

    def norm(c):
        r = rows_of(c)
        total = jnp.zeros((ROWS, span), F32)
        for a in range(QUARTERS):
            x = rv[a, r, :].astype(F32)
            total = total + x * x
        scale = lax.rsqrt(jnp.sum(total, axis=-1, keepdims=True) * (1.0 / width) + 1e-05)
        inv[r, :] = scale
        for a in range(QUARTERS):
            nv[a, r, :] = (rv[a, r, :].astype(F32) * scale * gain_f[a]).astype(BF16)

    def regroup():
        gq_t[...] = gqv[...].T
        for v in range(2):
            for j, rel in enumerate(((0, 2, 1, 3), (0, 1, 2, 3))[v]):
                y_to = yy + (rel // 2) * (1 - 2 * yy)
                x_to = xx + (rel % 2) * (1 - 2 * xx)
                for mine in range(2):
                    c_to = core if mine else 1 - core
                    at = pl.multiple_of((y_to * 4 + x_to * 2 + c_to) * block, block)
                    gq_p[v, mine, j * block:(j + 1) * block, :] = gq_t[pl.ds(at, block), :]

    first, second = (x_mate, y_mate), (y_mate, x_mate)

    def product(mine, j, v):
        return jnp.dot(gq_p[v, mine], nv[j, :, v * cols:(v + 1) * cols], preferred_element_type=F32)

    def stage1(j):
        for v in range(2):
            t = 2 * j + v
            fgs[t] = product(0, j, v).astype(BF16)
            hop(fgs, fgr, s1, r1, t, core_mate).start()

    def stage2(j):
        for v in range(2):
            t = 2 * j + v
            hop(fgs, fgr, s1, r1, t, core_mate).wait_recv()
            total = product(1, j, v) + fgr[t].astype(F32)
            xs[t] = total[2 * block:].astype(BF16)
            hop(xs, xr, s2, r2, t, first[v]).start()
            keep[t] = total[:2 * block]

    def stage3(j):
        for v in range(2):
            t = 2 * j + v
            hop(xs, xr, s2, r2, t, first[v]).wait_recv()
            ys[t] = (keep[t, block:] + xr[t, block:].astype(F32)).astype(BF16)
            hop(ys, yr, s3, r3, t, second[v]).start()
            keep[t, :block] = keep[t, :block] + xr[t, :block].astype(F32)

    def stage4(j):
        for v in range(2):
            t = 2 * j + v
            hop(ys, yr, s3, r3, t, second[v]).wait_recv()
            wgo[t] = keep[t, :block] + yr[t].astype(F32)

    def pass_on(c):
        r = rows_of(c)
        to_mate(part, from_mate, other, c).wait_recv()
        for q in range(2):
            at = (other, r, lanes_of(q))
            part[at] = (part[at].astype(F32) + from_mate[at].astype(F32)).astype(BF16)
        to_peer(part, from_peer, other, c).start()

    def root(c):
        r = rows_of(c)
        to_mate(part, from_mate, own, c).wait_recv()
        to_peer(part, from_peer, own, c).wait_recv()
        mine = jnp.minimum(c, last)
        keep_it = jnp.where(c == chunks, 0.0, 1.0)
        terms = []
        for q in range(2):
            at = (own, r, lanes_of(q))
            dnormed = part[at].astype(F32) + from_mate[at].astype(F32)
            dnormed = dnormed + from_peer[at].astype(F32)
            ds[at] = dnormed.astype(BF16)
            unit = rv[2 * own + q, rows_of(mine), :].astype(F32) * inv[rows_of(mine), :]
            terms.append(dnormed * unit * keep_it)
        to_mate(ds, ds, own, c).start()
        to_peer(ds, ds, own, c).start()
        for q in range(2):
            gacc[q] += terms[q][:8] + terms[q][8:]

    def forward(c):
        to_peer(ds, ds, other, c).wait_recv()
        to_mate(ds, ds, other, c).start()

    def give(half):
        return pltpu.make_async_remote_copy(
            src_ref=ds.at[half, rows_of(chunks)], dst_ref=ds.at[half, rows_of(last)],
            send_sem=sx.at[half], recv_sem=rx.at[half],
            device_id={"dp": core_mate}, device_id_type=MESH)

    def give_both():
        for half in range(2):
            give(half).start()

    def absorb():
        give(own).wait_recv()
        r = rows_of(last)
        for q in range(2):
            unit = rv[2 * own + q, r, :].astype(F32) * inv[r, :]
            term = ds[own, r, lanes_of(q)].astype(F32) * unit
            gacc[q] += term[:8] + term[8:]

    def collect(c):
        for half in range(2):
            to_mate(part, ds, half, c).wait_recv()

    def finish(c):
        r = rows_of(c)
        residual_rows(
            lambda a: ds[a // 2, r, lanes_of(a % 2)], lambda a: rv[a, r, :],
            lambda a: giv[a, r, :], inv[r, :], gain_f, gov, r)

    def g_copy(o):
        return pltpu.make_async_remote_copy(
            src_ref=gslot.at[0], dst_ref=gslot.at[o], send_sem=sg.at[o], recv_sem=rg.at[o],
            device_id={"dp": (dp + o) % n_dp}, device_id_type=MESH)

    targets = (mate, peer, (1 - h) * (n_tp - 1))

    def z_copy(i):
        return pltpu.make_async_remote_copy(
            src_ref=gz.at[h], dst_ref=gz.at[h], send_sem=sz.at[i], recv_sem=rz.at[h],
            device_id={"tp": targets[i]}, device_id_type=MESH)

    def z_wait(which):
        pltpu.make_async_remote_copy(
            src_ref=gz.at[which], dst_ref=gz.at[which], send_sem=sz.at[0], recv_sem=rz.at[which],
            device_id={"tp": mate}, device_id_type=MESH).wait_recv()

    def sent(sem):
        for which, rows in ((0, tokens - ROWS), (1, tokens + ROWS)):
            @pl.when(core == which)
            def _():
                pltpu.make_async_remote_copy(
                    src_ref=part.at[:, :rows], dst_ref=ds.at[:, :rows], send_sem=sem.at[0],
                    recv_sem=rm.at[0], device_id={"tp": mate}, device_id_type=MESH).wait_send()

    def at(i, lo, hi):
        return jnp.logical_and(i >= lo, i < hi)

    extra = jnp.logical_and(core == 1, is_inner)

    @pl.loop(0, chunks + LAG)
    def _(i):
        @pl.when(jnp.logical_and(is_inner, i < count))
        def _():
            pass_on(nth(i))

        @pl.when(jnp.logical_and(is_inner, at(i, 4, count + 4)))
        def _():
            forward(nth(i - 4))

        @pl.when(jnp.logical_and(extra, i == MIDDLE + 4))
        def _():
            give_both()

        @pl.when(jnp.logical_and(jnp.logical_and(is_inner, core == 0), i == chunks - 1))
        def _():
            absorb()

        @pl.when(jnp.logical_and(is_inner, at(i, 2, count + 2)))
        def _():
            root(nth(i - 2))

        @pl.when(jnp.logical_and(is_inner, i == count + 1))
        def _():
            for q in range(2):
                gslot[0, q:q + 1, :] = jnp.sum(gacc[q], axis=0, keepdims=True)
            for o in range(1, n_dp):
                g_copy(o).start()

        @pl.when(jnp.logical_and(is_inner, at(i, 5, count + 5)))
        def _():
            pl.when(nth(i - 5) < last)(lambda: finish(nth(i - 5)))

        @pl.when(jnp.logical_and(is_outer, at(i, LAG, last + core + LAG)))
        def _():
            collect(nth(i - LAG))
            pl.when(nth(i - LAG) < last)(lambda: finish(nth(i - LAG)))
            pl.when(nth(i - LAG) == chunks)(give_both)

        @pl.when(i == 0)
        def _():
            pl.loop(0, 5)(norm)

        @pl.when(i == 1)
        def _():
            pl.loop(5, 11)(norm)

        @pl.when(i == 3)
        def _():
            rv_end[...] = rv[:, tokens - ROWS:, :]
            gi_end[...] = giv[:, tokens - ROWS:, :]
            inv_end[...] = inv[tokens - ROWS:, :]

        @pl.when(i == 2)
        def _():
            pl.loop(11, chunks)(norm)
            regroup()

        @pl.when(at(i, 3, 5))
        def _():
            stage1(2 * (i - 3))
            stage1(2 * (i - 3) + 1)

        @pl.when(at(i, 5, 9))
        def _():
            stage2(i - 5)

        @pl.when(at(i, 9, 13))
        def _():
            stage3(i - 9)

        @pl.when(at(i, 13, 17))
        def _():
            stage4(i - 13)

    @pl.when(is_inner)
    def _():
        for o in range(1, n_dp):
            g_copy(o).wait_recv()
        total = gslot[dp % n_dp]
        for d in range(1, n_dp):
            total = total + gslot[(dp + n_dp - d) % n_dp]
        gz[h] = total
        for i in range(3):
            z_copy(i).start()
        z_wait(1 - h)
        for i in range(3):
            z_copy(i).wait_send()
        for o in range(1, n_dp):
            g_copy(o).wait_send()
        sent(sp)

    pl.when(jnp.logical_and(is_outer, core == 1))(lambda: collect(last))

    @pl.when(core == 0)
    def _():
        ends.wait_send()
        pl.when(is_outer)(lambda: give(own).wait_recv())
        give(other).wait_recv()

    @pl.when(core == 1)
    def _():
        for half in range(2):
            give(half).wait_send()

    ds_end[...] = ds[:, tokens - ROWS:tokens, :]

    @pl.when(is_outer)
    def _():
        z_wait(0)
        z_wait(1)

    for a in range(QUARTERS):
        ggv[:, a * span:(a + 1) * span] = gz[a // 2, a % 2:a % 2 + 1, :]
    sent(so)

    for t in range(TILES):
        hop(fgs, fgr, s1, r1, t, core_mate).wait_send()
        hop(xs, xr, s2, r2, t, first[t % 2]).wait_send()
        hop(ys, yr, s3, r3, t, second[t % 2]).wait_send()


def write_out(wgo, ggv, gov, ds_end, rv_end, gi_end, inv_end, gain_f,
              wg_out, gg_out, go_out, end, sem):
    cols, span = wgo.shape[2], gov.shape[2]
    done = gov.shape[1] - ROWS
    copies = [
        pltpu.make_async_copy(
            gov.at[a, :done], go_out.at[:done, a * span:(a + 1) * span], sem.at[a])
        for a in range(QUARTERS)
    ]
    copies += [
        pltpu.make_async_copy(
            wgo.at[t], wg_out.at[:, t * cols:(t + 1) * cols], sem.at[QUARTERS + t])
        for t in range(TILES)
    ]
    copies.append(pltpu.make_async_copy(ggv, gg_out, sem.at[QUARTERS + TILES]))
    for copy in copies:
        copy.start()
    residual_rows(
        lambda a: ds_end[a // 2, :, a % 2 * span:(a % 2 + 1) * span], lambda a: rv_end[a],
        lambda a: gi_end[a], inv_end[...], gain_f, end, slice(0, ROWS))
    for a in range(QUARTERS):
        copies.append(pltpu.make_async_copy(
            end.at[a], go_out.at[done:, a * span:(a + 1) * span],
            sem.at[QUARTERS + TILES + 1 + a]))
        copies[-1].start()
    for copy in copies:
        copy.wait()


def fused(n_dp, n_tp, resid, gain, grad_q, w_query, grad_in):
    tokens, width = resid.shape
    heads = grad_q.shape[1]
    chunks = tokens // ROWS
    block, cols, span = heads // n_dp, width // TILES, width // QUARTERS
    any_space = pl.BlockSpec(memory_space=pl.ANY)
    dma = lambda n: pltpu.SemaphoreType.DMA((n,))
    wide = lambda: pltpu.VMEM((QUARTERS, tokens, span), BF16)
    halves = lambda: pltpu.VMEM((2, tokens + ROWS, 2 * span), BF16)
    vmem = pl.BlockSpec(memory_space=pltpu.VMEM)
    held = pl.pallas_call(
        functools.partial(kernel, n_dp, n_tp),
        out_shape=(
            pltpu.VMEM((TILES, block, cols), F32),
            pltpu.VMEM((1, width), F32),
            pltpu.VMEM((QUARTERS, tokens, span), BF16),
            pltpu.VMEM((2, ROWS, 2 * span), BF16),
            pltpu.VMEM((QUARTERS, ROWS, span), BF16),
            pltpu.VMEM((QUARTERS, ROWS, span), BF16),
            pltpu.VMEM((ROWS, 1), F32),
            pltpu.VMEM((QUARTERS, 1, span), F32),
        ),
        in_specs=[any_space] * 5,
        out_specs=(vmem,) * 8,
        scratch_shapes=[
            pltpu.VMEM((QUARTERS, heads, span), BF16),
            wide(),
            pltpu.VMEM((tokens, heads), BF16),
            wide(), wide(), halves(), halves(), halves(), halves(),
            pltpu.VMEM((width // 128, 128), BF16),
            pltpu.VMEM((tokens, 1), F32),
            pltpu.VMEM((heads, tokens), BF16),
            pltpu.VMEM((2, 2, 4 * block, tokens), BF16),
            pltpu.VMEM((TILES, 4 * block, cols), BF16),
            pltpu.VMEM((TILES, 4 * block, cols), BF16),
            pltpu.VMEM((TILES, 2 * block, cols), F32),
            pltpu.VMEM((TILES, 2 * block, cols), BF16),
            pltpu.VMEM((TILES, 2 * block, cols), BF16),
            pltpu.VMEM((TILES, block, cols), BF16),
            pltpu.VMEM((TILES, block, cols), BF16),
            pltpu.VMEM((2, 8, span), F32),
            pltpu.VMEM((n_dp, 2, span), F32),
            pltpu.VMEM((2, 2, span), F32),
            pltpu.VMEM((ROWS, heads), BF16),
            dma(QUARTERS), dma(3), dma(QUARTERS), dma(QUARTERS), dma(1), dma(1),
            dma(2 * chunks + 2), dma(2 * chunks + 2), dma(1), dma(1), dma(2), dma(2),
            dma(TILES), dma(TILES), dma(TILES), dma(TILES), dma(TILES), dma(TILES),
            dma(n_dp), dma(n_dp), dma(3), dma(2),
        ],
        compiler_params=pltpu.CompilerParams(
            collective_id=0, has_side_effects=True, vmem_limit_bytes=VMEM_MIB * 1024 * 1024
        ),
    )(resid, gain.reshape(width // 128, 128), grad_q, w_query, grad_in)
    weight_grad, gain_grad, grad_rows = pl.pallas_call(
        write_out,
        out_shape=(
            jax.ShapeDtypeStruct((block, width), F32),
            jax.ShapeDtypeStruct((1, width), F32),
            jax.ShapeDtypeStruct((tokens, width), BF16),
        ),
        in_specs=[vmem] * 8,
        out_specs=(any_space,) * 3,
        scratch_shapes=[
            pltpu.VMEM((QUARTERS, ROWS, span), BF16), dma(TILES + 2 * QUARTERS + 1)],
        compiler_params=pltpu.CompilerParams(vmem_limit_bytes=2 * 1024 * 1024),
    )(*held)
    return weight_grad, gain_grad.reshape(width), grad_rows


def solution(mesh):
    n_dp, n_tp = mesh.shape["dp"], mesh.shape["tp"]
    if (n_dp, n_tp) == (2 * 2 * 2, 4):
        body = functools.partial(fused, n_dp, n_tp)
    else:
        body = per_device
    return jax.shard_map(
        body,
        mesh=mesh,
        in_specs=(P("dp", None), P(), P("dp", "tp"), P("tp", None), P("dp", None)),
        out_specs=(P(("tp", "dp"), None), P(), P("dp", None)),
        check_vma=False,
    )
```
